32 devices in a mesh: grp: 8 (over y, x, core), tile: 4 (over z).
Axes of the slice: x: 2, y: 2, z: 4, core: 2. Of those that a mesh axis runs over, the one named last changes fastest.
Arguments:
- atm_flux: float32 [6, 32768], P(None, ('grp', 'tile')), may hold values from -6 to 6
- send_block: int32 [32, 4, 4], P(('grp', 'tile')), may hold values from 0 to 7
- send_count: int32 [32, 4], P(('grp', 'tile')), may hold values from 1 to 4, as said below
- recv_block: int32 [32, 4, 4], P(('grp', 'tile')), may hold values from 0 to 63
- recv_weight: bfloat16 [32, 4, 4, 128, 128], P(('grp', 'tile')), may hold values from -0.5 to 0.5
- sea_temp: float32 [256, 1024], P('grp', 'tile'), may hold values from -6 to 6
- ocean_mask: int32 [256, 1024], P('grp', 'tile'), may hold values 0 or 1
Outputs:
- heat_flux: float32 [256, 1024], P('grp', 'tile')
- stress_curl: float32 [256, 1024], P('grp', 'tile')
- atm_return: float32 [4, 32768], P(None, ('grp', 'tile'))
The draws below stay inside these ranges and needn't reach their ends.
Inputs may be any that keep to these rules, and one draw needn't show every extreme that they name: `send_count`: in every draw a quarter of the tile indices, drawn from the seed, receive exactly 4 blocks from every device of their group; every other pair carries 1 to 2 blocks.
All inputs are finite; a program needn't handle non-finite values. No bound on the sum of `ocean_mask` on one device may be relied on, other than what follows from the above.
Results may differ from the reference program's by a relative error of at most 0.0003.
Values sent between devices are 32-bit elements; how exact they have to be, the bound alone decides.
No kernel may reach another device: no remote copies, remote signals or barrier semaphores. Data moves between devices by JAX's collectives and lax.ppermute only.
A program may use at most 64 MiB of HBM per device.

```python
import jax
import jax.numpy as jnp
from jax import lax

NF = 6
NB = 4
BLK = 128
CAP = 4
ABLK_DEV = 8
OROW = 32
OCOL = 256
OBLK = 64
NYO = 256
NXO = 1024
ACELLS = 32768
N_GRP = 8
N_TILE = 4
DEVICES = 32


def draw_send_count(key, part):
    first_key, second_key = jax.random.split(jax.random.fold_in(key, 11))
    base_count = jax.random.randint(first_key, (DEVICES, N_TILE), 1, CAP // 2 + 1)
    offset = jax.random.randint(second_key, (), 0, 4)
    column = jnp.arange(N_TILE, dtype=jnp.int32)
    busy = ((column + offset) % 4 == 0)[None, :]
    return jnp.where(busy, CAP, base_count).astype(jnp.int32)


def set_ends(drawn, key, least, high):
    longest = drawn.shape.index(max(drawn.shape))
    spots = []
    for shift in (0, 1):
        where = [jax.random.randint(jax.random.fold_in(key, axis), (), 0, length) for axis, length in enumerate(drawn.shape)]
        where[longest] = (where[longest] + shift) % drawn.shape[longest]
        spots.append(tuple(where))
    return drawn.at[spots[0]].set(least).at[spots[1]].set(high)


def shard_levels(stream_key, extent, cuts, smallest, largest):
    def one(dim, parts):
        heights = jax.random.uniform(jax.random.fold_in(jax.random.fold_in(stream_key, 6), dim), (parts,), jnp.float32, smallest / len(cuts), largest / len(cuts))
        return jnp.repeat(jnp.exp(heights), extent[dim] // parts).reshape((-1,) + (1,) * (len(extent) - dim - 1))

    loudness = one(*cuts[0])
    for cut in cuts[1:]:
        loudness = loudness * one(*cut)
    return loudness


def noise(key, extent, deviation, reach, cuts=(), kind=jnp.bfloat16):
    values = deviation * jax.random.normal(key, extent, jnp.float32)
    if cuts:
        values = values * shard_levels(key, extent, cuts, -0.22, 0.18)
    return jnp.clip(values, -reach, reach).astype(kind)


def setup_inputs(seed: int = 0) -> dict:
    key_of = jax.random.split(jax.random.key(seed), 8)
    return {
        "atm_flux": noise(key_of[0], (NF, ACELLS), 1.0, 6.0, ((1, 32),), jnp.float32),
        "send_block": set_ends(jax.random.randint(key_of[1], (DEVICES, N_TILE, CAP), 0, ABLK_DEV), jax.random.fold_in(key_of[1], 1), 0, ABLK_DEV - 1).astype(jnp.int32),
        "send_count": draw_send_count(jax.random.fold_in(key_of[7], 71), 0),
        "recv_block": set_ends(jax.random.randint(key_of[3], (DEVICES, N_TILE, CAP), 0, OBLK), jax.random.fold_in(key_of[3], 1), 0, OBLK - 1).astype(jnp.int32),
        "recv_weight": noise(key_of[4], (DEVICES, N_TILE, CAP, BLK, BLK), BLK ** -0.5, 0.5, ((0, 32),)),
        "sea_temp": noise(key_of[5], (NYO, NXO), 1.0, 6.0, ((0, 8), (1, 4)), jnp.float32),
        "ocean_mask": set_ends((jax.random.randint(key_of[6], (NYO, NXO), 0, 10) < 7).astype(jnp.int32), jax.random.fold_in(key_of[6], 1), 0, 1),
    }


precise = lax.Precision.HIGHEST

def bulk_formula(fields, surface_temp, ocean_mask):
    sea_share = ocean_mask.astype(jnp.float32)
    wind_u, wind_v, air_temp, air_vapor, short_down, long_down = [fields[k] for k in range(6)]
    wind_speed = jnp.sqrt(wind_u * wind_u + wind_v * wind_v + 0.5)
    stress_x = 0.8 * wind_speed * wind_u * sea_share
    stress_y = 0.8 * wind_speed * wind_v * sea_share
    sensible = 0.6 * wind_speed * (surface_temp - air_temp)
    latent = 0.7 * wind_speed * (jnp.exp(0.3 * surface_temp) - air_vapor)
    long_up = 0.4 * (1.0 + 0.2 * surface_temp) ** 4
    heat_flux = (0.94 * short_down + long_down - long_up - sensible - latent) * sea_share
    surface = jnp.stack([surface_temp, sensible, latent, long_up]) * sea_share[None]
    return (stress_x, stress_y, heat_flux, surface)

def reference(atm_flux, send_block, send_count, recv_block, recv_weight, sea_temp, ocean_mask):
    group_count = N_GRP
    tile_count = N_TILE
    device_count = group_count * tile_count
    slot_range = jnp.arange(CAP, dtype=jnp.int32)
    blocks = atm_flux.reshape(NF, device_count, ABLK_DEV, BLK)

    def pick_slots(dev_blocks, send_index, pair_count):
        chosen = jnp.take(dev_blocks, send_index, axis=1)
        live_slots = (slot_range[None, :] < pair_count[:, None]).astype(jnp.float32)
        return chosen * live_slots[None, :, :, None]
    picked = jax.vmap(pick_slots, in_axes=(1, 0, 0))(blocks, send_block, send_count)
    picked = picked.reshape(group_count, tile_count, NF, tile_count, CAP, BLK)
    arrived = jnp.transpose(picked, (0, 3, 1, 4, 2, 5)).reshape(device_count, tile_count, CAP, NF, BLK)

    def remap_in(entries):
        weight, dest_block, incoming = entries
        weight_wide = weight.astype(jnp.float32)
        remapped = jnp.einsum('scij,scfj->scfi', weight_wide, incoming, precision=precise)
        onehot = (jnp.arange(OBLK, dtype=jnp.int32)[:, None] == dest_block.reshape(-1)[None, :]).astype(jnp.float32)
        landed = jnp.dot(onehot, remapped.reshape(tile_count * CAP, NF * BLK), precision=precise)
        return landed.reshape(OBLK, NF, BLK)
    landed = lax.map(remap_in, (recv_weight, recv_block, arrived))
    grid = landed.reshape(group_count, tile_count, OBLK, NF, BLK).transpose(3, 0, 1, 2, 4)
    grid = grid.reshape(NF, group_count, tile_count, OROW, OCOL).transpose(0, 1, 3, 2, 4).reshape(NF, NYO, NXO)
    stress_x, stress_y, heat_flux, surface = bulk_formula(grid, sea_temp, ocean_mask)
    sea_share = ocean_mask.astype(jnp.float32)
    fold_values = -jnp.flip(stress_x[NYO - 1])
    column_x = jnp.concatenate([jnp.zeros((1, NXO), jnp.float32), stress_x, fold_values[None]], axis=0)
    stress_curl = 0.5 * (jnp.roll(stress_y, -1, axis=1) - jnp.roll(stress_y, 1, axis=1)) - 0.5 * (column_x[2:] - column_x[:-2])
    stress_curl = stress_curl * sea_share
    per_device = surface.reshape(NB, group_count, OROW, tile_count, OCOL).transpose(1, 3, 0, 2, 4)
    per_device = per_device.reshape(device_count, NB, OBLK, BLK)

    def remap_out(entries):
        weight, dest_block, ocean_blocks = entries
        weight_wide = weight.astype(jnp.float32)
        chosen = jnp.take(ocean_blocks, dest_block, axis=1)
        return jnp.einsum('scij,fsci->scfj', weight_wide, chosen, precision=precise)
    returned = lax.map(remap_out, (recv_weight, recv_block, per_device))
    returned = returned.reshape(group_count, tile_count, tile_count, CAP, NB, BLK).transpose(0, 2, 1, 3, 4, 5)
    returned = returned.reshape(device_count, tile_count, CAP, NB, BLK)

    def gather_back(send_index, pair_count, pieces):
        live_slots = (slot_range[None, :] < pair_count[:, None]).astype(jnp.float32)
        pieces = pieces * live_slots[:, :, None, None]
        onehot = (jnp.arange(ABLK_DEV, dtype=jnp.int32)[:, None] == send_index.reshape(-1)[None, :]).astype(jnp.float32)
        total = jnp.dot(onehot, pieces.reshape(tile_count * CAP, NB * BLK), precision=precise)
        return total.reshape(ABLK_DEV, NB, BLK)
    atm_parts = jax.vmap(gather_back)(send_block, send_count, returned)
    atm_return = atm_parts.transpose(2, 0, 1, 3).reshape(NB, ACELLS)
    return (heat_flux, stress_curl, atm_return)
```

```python
import functools

import jax
import jax.numpy as jnp
from jax import lax
from jax.experimental import pallas as pl
from jax.experimental.pallas import tpu as pltpu
from jax.sharding import PartitionSpec as P

SUB = 8
F32 = jnp.float32
BF16 = jnp.bfloat16
VMEM = pl.BlockSpec(memory_space=pltpu.VMEM)
SMEM = pl.BlockSpec(memory_space=pltpu.SMEM)
PARAMS = pltpu.CompilerParams(vmem_limit_bytes=4 * 1024 * 1024)


def round_up(value, unit):
    return -(-value // unit) * unit


def is_column_mask(mask):
    return mask > 0 and mask & (mask + 1) == 0


def pack_kernel(send_block, send_count, atm_flux, *outs):
    here = lax.axis_index("tile")
    field_count = atm_flux.shape[0]
    slot_count, rows, cells = outs[0].shape
    for mask, out in enumerate(outs):
        peer = here ^ mask
        count = send_count[0, peer]
        for slot in range(slot_count):
            start = pl.multiple_of(send_block[0, peer, slot] * cells, cells)
            chosen = atm_flux[:, pl.ds(start, cells)]
            out[slot, :field_count, :] = jnp.where(slot < count, chosen, 0.0)
            if rows > field_count:
                out[slot, field_count:, :] = jnp.zeros((rows - field_count, cells), F32)


def split(value):
    high = value.astype(BF16)
    low = (value - high.astype(F32)).astype(BF16)
    return high, low


def middle_kernel(tile_count, field_count, back_count, recv_block, weight, sea_temp, ocean_mask, *refs):
    arrived = refs[:tile_count]
    heat, stress_x, stress_y, even_row, odd_row = refs[tile_count : tile_count + 5]
    payload = refs[tile_count + 5 : 2 * tile_count + 5]
    landed, surface = refs[2 * tile_count + 5 :]
    here = lax.axis_index("tile")
    slot_count, field_rows, cells = arrived[0].shape
    rows, cols = sea_temp.shape
    halves = cols // cells
    tiles = rows // SUB
    pairs = [(mask, slot) for mask in range(tile_count) for slot in range(slot_count)]
    landed[...] = jnp.zeros_like(landed)
    for mask, slot in pairs:
        source = here ^ mask
        high, low = split(arrived[mask][slot])
        both = jnp.concatenate([high, low], axis=0)
        result = lax.dot_general(
            both, weight[0, source, slot], (((1,), (1,)), ((), ())), preferred_element_type=F32
        )
        start = pl.multiple_of(recv_block[0, source, slot] * field_rows, field_rows)
        landed[pl.ds(start, field_rows), :] += result[:field_rows] + result[field_rows:]
    surface_rows = surface.shape[0] // (rows * halves)
    lane = lax.broadcasted_iota(jnp.int32, (SUB, cells), 1)
    edge = jnp.zeros((SUB, cells), F32)
    for half in range(halves):
        span = slice(half * cells, (half + 1) * cells)
        fields = [
            landed[pl.ds(half * field_rows + k, rows, stride=halves * field_rows), :]
            for k in range(field_count)
        ]
        wind_u, wind_v, air_temp, air_vapor, short_down, long_down = fields
        temp = sea_temp[:, span]
        share = ocean_mask[:, span].astype(F32)
        speed = jnp.sqrt(wind_u * wind_u + wind_v * wind_v + 0.5)
        drag = 0.8 * speed * share
        along_x = drag * wind_u
        along_y = drag * wind_v
        sensible = 0.6 * speed * (temp - air_temp)
        latent = 0.7 * speed * (jnp.exp(0.3 * temp) - air_vapor)
        base = 1.0 + 0.2 * temp
        square = base * base
        long_up = 0.4 * (square * square)
        heat[:, span] = (0.94 * short_down + long_down - long_up - sensible - latent) * share
        stress_x[:, span] = along_x
        stress_y[:, span] = along_y
        even_row[half : half + 1, :] = along_x[rows - 1 :]
        odd_row[half : half + 1, :] = along_x[:1]
        for k, value in enumerate([temp, sensible, latent, long_up]):
            value = value * share
            high = value.astype(BF16).astype(F32)
            step = halves * surface_rows
            surface[pl.ds(half * surface_rows + k, rows, stride=step), :] = high
            surface[pl.ds(half * surface_rows + back_count + k, rows, stride=step), :] = value - high
        if half == 0:
            for q in range(tiles):
                part = along_y[q * SUB : (q + 1) * SUB]
                edge = jnp.where(lane == q, pltpu.roll(part, q, 1), edge)
        if half == halves - 1:
            for q in range(tiles):
                part = along_y[q * SUB : (q + 1) * SUB]
                moved = pltpu.roll(part, (tiles + q + 1) % cells, 1)
                edge = jnp.where(lane == tiles + q, moved, edge)
    back_rows = slot_count * back_count
    for mask in range(tile_count):
        if is_column_mask(mask):
            payload[mask][back_rows : back_rows + SUB, :] = edge
        if mask == tile_count - 1:
            payload[mask][back_rows + SUB : back_rows + SUB + halves, :] = even_row[...]
    odd = lax.axis_index("grp") % 2 == 1
    top, bottom = even_row[...], odd_row[...]
    even_row[...] = jnp.where(odd, bottom, top)
    odd_row[...] = jnp.where(odd, top, bottom)
    for mask, slot in pairs:
        source = here ^ mask
        start = pl.multiple_of(recv_block[0, source, slot] * surface_rows, surface_rows)
        chosen = surface[pl.ds(start, surface_rows), :].astype(BF16)
        result = jnp.dot(chosen, weight[0, source, slot], preferred_element_type=F32)
        payload[mask][slot * back_count : (slot + 1) * back_count, :] = (
            result[:back_count] + result[back_count : 2 * back_count]
        )


def final_kernel(tile_count, back_count, send_block, send_count, ocean_mask, stress_x, stress_y, near, far, *refs):
    payload = refs[:tile_count]
    curl, atm = refs[tile_count:]
    here = lax.axis_index("tile")
    group = lax.axis_index("grp")
    group_count = lax.axis_size("grp")
    rows, cols = stress_x.shape
    cells = payload[0].shape[1]
    slot_count = send_block.shape[2]
    back_rows = slot_count * back_count
    halves = cols // cells
    tiles = rows // SUB
    odd = group % 2 == 1
    south = jnp.where(odd, near[...], far[...])
    south = jnp.where(group == 0, 0.0, south)
    north = jnp.where(odd, far[...], near[...])
    fold = payload[tile_count - 1][back_rows + SUB : back_rows + SUB + halves, :]
    turn = cells - 1 - lax.broadcasted_iota(jnp.int32, (SUB, cells), 1)
    last = group == group_count - 1
    east_edge = jnp.zeros((SUB, cells), F32)
    west_edge = jnp.zeros((SUB, cells), F32)
    east_mask = here ^ ((here + 1) % tile_count)
    west_mask = here ^ ((here + tile_count - 1) % tile_count)
    for mask in range(tile_count):
        if is_column_mask(mask):
            value = payload[mask][back_rows : back_rows + SUB, :]
            east_edge = jnp.where(east_mask == mask, value, east_edge)
            west_edge = jnp.where(west_mask == mask, value, west_edge)
    east_halo = jnp.concatenate([pltpu.roll(east_edge, cells - 1 - q, 1) for q in range(tiles)], axis=0)
    west_halo = jnp.concatenate([pltpu.roll(west_edge, cells - tiles - q, 1) for q in range(tiles)], axis=0)
    lane = lax.broadcasted_iota(jnp.int32, (rows, cells), 1)
    row = lax.broadcasted_iota(jnp.int32, (rows, cells), 0)
    parts = [stress_y[:, half * cells : (half + 1) * cells] for half in range(halves)]
    ahead = [pltpu.roll(part, cells - 1, 1) for part in parts] + [east_halo]
    behind = [west_halo] + [pltpu.roll(part, 1, 1) for part in parts]
    for half in range(halves):
        span = slice(half * cells, (half + 1) * cells)
        mirrored = jnp.broadcast_to(fold[halves - 1 - half][None], (SUB, cells))
        mirrored = jnp.take_along_axis(mirrored, turn, axis=1)[:1]
        above = jnp.where(last, -mirrored, north[half][None])
        below = south[half][None]
        east = jnp.where(lane == cells - 1, ahead[half + 1], ahead[half])
        west = jnp.where(lane == 0, behind[half], behind[half + 1])
        part = stress_x[:, span]
        up = jnp.where(row == rows - 1, above, pltpu.roll(part, rows - 1, 0))
        down = jnp.where(row == 0, below, pltpu.roll(part, 1, 0))
        share = ocean_mask[:, span].astype(F32)
        curl[:, span] = (0.5 * (east - west) - 0.5 * (up - down)) * share
    atm[...] = jnp.zeros_like(atm)
    for mask in range(tile_count):
        peer = here ^ mask
        count = send_count[0, peer]
        for slot in range(slot_count):
            start = pl.multiple_of(send_block[0, peer, slot] * cells, cells)
            value = payload[mask][slot * back_count : (slot + 1) * back_count, :]
            atm[:, pl.ds(start, cells)] += jnp.where(slot < count, value, 0.0)


def per_device(atm_flux, send_block, send_count, recv_block, recv_weight, sea_temp, ocean_mask):
    tile_count = lax.axis_size("tile")
    group_count = lax.axis_size("grp")
    field_count = atm_flux.shape[0]
    slot_count = send_block.shape[2]
    cells = recv_weight.shape[-1]
    rows, cols = sea_temp.shape
    halves = cols // cells
    back_count = 4
    field_rows = round_up(field_count, SUB)
    surface_rows = round_up(2 * back_count, SUB)
    back_rows = slot_count * back_count
    shape = jax.ShapeDtypeStruct

    def swap(value, mask):
        return lax.ppermute(value, "tile", [(i, i ^ mask) for i in range(tile_count)])

    packed = pl.pallas_call(
        pack_kernel,
        out_shape=[shape((slot_count, field_rows, cells), F32)] * tile_count,
        in_specs=[SMEM, SMEM, VMEM],
        out_specs=[VMEM] * tile_count,
        compiler_params=PARAMS,
        name="pack",
    )(send_block, send_count, atm_flux)
    arrived = list(packed)
    for mask in reversed(range(1, tile_count)):
        arrived[mask] = swap(packed[mask], mask)

    def payload_rows(mask):
        extra = SUB if is_column_mask(mask) else 0
        return back_rows + extra + (halves if mask == tile_count - 1 else 0)

    outs = pl.pallas_call(
        functools.partial(middle_kernel, tile_count, field_count, back_count),
        out_shape=[shape((rows, cols), F32)] * 3
        + [shape((halves, cells), F32)] * 2
        + [shape((payload_rows(mask), cells), F32) for mask in range(tile_count)],
        in_specs=[SMEM] + [VMEM] * (3 + tile_count),
        out_specs=[VMEM] * (5 + tile_count),
        scratch_shapes=[
            pltpu.VMEM((rows * halves * field_rows, cells), F32),
            pltpu.VMEM((rows * halves * surface_rows, cells), F32),
        ],
        compiler_params=PARAMS,
        name="middle",
    )(recv_block, recv_weight, sea_temp, ocean_mask, *arrived)
    heat, stress_x, stress_y, near, far = outs[:5]
    payload = list(outs[5:])
    far = lax.ppermute(
        far, "grp", [(i, i + 1 if i % 2 else i - 1) for i in range(1, group_count - 1)]
    )
    for mask in reversed(range(1, tile_count)):
        payload[mask] = swap(payload[mask], mask)
    near = lax.ppermute(near, "grp", [(i, i ^ 1) for i in range(group_count)])
    curl, atm = pl.pallas_call(
        functools.partial(final_kernel, tile_count, back_count),
        out_shape=[shape((rows, cols), F32), shape((back_count, atm_flux.shape[1]), F32)],
        in_specs=[SMEM, SMEM] + [VMEM] * (5 + tile_count),
        out_specs=[VMEM] * 2,
        compiler_params=PARAMS,
        name="final",
    )(send_block, send_count, ocean_mask, stress_x, stress_y, near, far, *payload)
    return (heat, curl, atm)


def solution(mesh):
    placed = (
        P(None, ("grp", "tile")),
        P(("grp", "tile"), None, None),
        P(("grp", "tile"), None),
        P(("grp", "tile"), None, None),
        P(("grp", "tile"), None, None, None, None),
        P("grp", "tile"),
        P("grp", "tile"),
    )
    return jax.shard_map(
        per_device,
        mesh=mesh,
        in_specs=placed,
        out_specs=(P("grp", "tile"), P("grp", "tile"), P(None, ("grp", "tile"))),
        check_vma=False,
    )
```
